32 devices in a mesh: dp: 16 (over z, y, x), tensor: 2 (over core).
Axes of the slice: x: 2, y: 2, z: 4, core: 2. Of those that a mesh axis runs over, the one named last changes fastest.
Arguments:
- gradient: bfloat16 [16, 128, 8192], P('dp', 'tensor'), may hold values from -110 to 110
- momentum: bfloat16 [16, 128, 8192], P('dp', 'tensor'), may hold values from -6 to 6
- indices: int32 [16, 2, 128, 32], P('dp', 'tensor'), may hold values from 0 to 4095, all different within a row
Outputs:
- new_momentum: bfloat16 [16, 128, 8192], P('dp', 'tensor')
- update: bfloat16 [128, 8192], P('tensor')
The draws below stay inside these ranges and needn't reach their ends.
Inputs may be any that keep to these rules, and one draw needn't show every extreme that they name: The 32 indices of one span of one replica are distinct; index a * 64 + b names row frequency a and column frequency b.
All inputs are finite; a program needn't handle non-finite values.
Results may differ from the reference program's by a relative error of at most 0.0049.
Values may be sent and summed in bfloat16 or wider, within the bound.
A program may use at most 64 MiB of HBM per device.

```python
import jax
import jax.numpy as jnp
from jax import lax

D = 8192
BLOCK = 64
TOPK = 32
ROWS = 128
REPLICAS = 16


def draw_gradient(key, part):
    keys = jax.random.split(key, 3)
    own = jnp.clip(jax.random.normal(keys[0], (REPLICAS, ROWS, D), jnp.float32), -4.0, 4.0)
    position = jnp.arange(ROWS, dtype=jnp.float32) / ROWS
    rough_rows = jax.random.uniform(keys[1], (ROWS,), jnp.float32, 0.5, 2.0)
    rough_cols = jax.random.uniform(keys[2], (D,), jnp.float32, 0.5, 2.0)
    ramp = 10.0 ** (position - 0.5) * rough_rows
    return (own * ramp[None, :, None] * rough_cols[None, None, :]).astype(jnp.bfloat16)


def levels(rng, extent, shards, least, largest):
    gain, own = 1.0, jax.random.fold_in(rng, 6)
    for dim, parts in shards:
        heights = jnp.exp(jax.random.uniform(jax.random.fold_in(own, dim), (parts,), jnp.float32, least / len(shards), largest / len(shards)))
        gain = gain * jnp.repeat(heights, extent[dim] // parts).reshape([-1 if axis == dim else 1 for axis in range(len(extent))])
    return gain


def choose_distinct(key, rows, amount, top, lift):
    sequence = jax.random.permutation(jax.random.fold_in(key, 1), amount)
    pull = sequence
    for power in range(3):
        pull = pull * pull // amount
    pull = pull * lift // amount
    lots = jax.random.randint(jax.random.fold_in(key, 2), (rows, amount), 0, 4096) + pull
    sure = jax.random.permutation(jax.random.fold_in(key, 3), rows)[jnp.arange(amount) % rows]
    lots = jnp.where(jnp.arange(rows)[:, None] == sure[None, :], 1 << 14, lots)
    priority = lots * amount + jnp.arange(amount)
    return lax.top_k(priority.astype(jnp.int32), top)[1].astype(jnp.int32)


def noise(rng, extent, width, limit, shards=(), kind=jnp.bfloat16):
    loudness = levels(rng, extent, shards, -0.22, 0.18) if shards else 1.0
    array = jax.random.normal(rng, extent, jnp.float32) * width * loudness
    return jnp.minimum(jnp.maximum(array, -limit), limit).astype(kind)


def setup_inputs(seed: int = 0) -> dict:
    arg_keys = jax.random.split(jax.random.key(seed), 4)
    gradient = draw_gradient(jax.random.fold_in(arg_keys[3], 71), 0)
    momentum = noise(arg_keys[1], (REPLICAS, ROWS, D), 1.0, 6.0, ((0, 16), (1, 2)))
    indices = choose_distinct(arg_keys[2], REPLICAS * (ROWS // BLOCK) * (D // BLOCK), BLOCK * BLOCK, TOPK, 0).reshape((REPLICAS, ROWS // BLOCK, D // BLOCK, TOPK))
    return dict(gradient=gradient, momentum=momentum, indices=indices)


EPSILON = 1e-06
DECAY = 0.999

def dct_basis(block_edge):
    frequency = jnp.arange(block_edge, dtype=jnp.float32)[:, None]
    position = jnp.arange(block_edge, dtype=jnp.float32)[None, :]
    waves = jnp.cos(jnp.pi * (2.0 * position + 1.0) * frequency / (2.0 * block_edge))
    weights = jnp.where(frequency == 0.0, jnp.sqrt(1.0 / block_edge), jnp.sqrt(2.0 / block_edge))
    return waves * weights

def reference(gradient, momentum, indices):
    cosines = dct_basis(BLOCK)
    row_blocks = ROWS // BLOCK
    col_blocks = D // BLOCK
    precise = lax.Precision.HIGHEST
    block_rows = jnp.arange(row_blocks, dtype=jnp.int32)[:, None, None]
    block_cols = jnp.arange(col_blocks, dtype=jnp.int32)[None, :, None]

    def to_spans(slab):
        return slab.reshape(row_blocks, BLOCK, col_blocks, BLOCK).transpose(0, 2, 1, 3)

    def from_spans(blocks):
        return blocks.transpose(0, 2, 1, 3).reshape(ROWS, D)

    def compress(operands):
        grad_slab, moment_slab, chosen = operands
        renewed = DECAY * moment_slab.astype(jnp.float32) + grad_slab.astype(jnp.float32)
        spectrum = jnp.einsum('ka,pqab,lb->pqkl', cosines, to_spans(renewed), cosines, precision=precise)
        flattened = spectrum.reshape(row_blocks, col_blocks, BLOCK * BLOCK)
        picked = jnp.take_along_axis(flattened, chosen, axis=2)
        marker = jnp.zeros_like(flattened).at[block_rows, block_cols, chosen].set(1.0)
        retained = (flattened * marker).reshape(row_blocks, col_blocks, BLOCK, BLOCK)
        restored = jnp.einsum('ka,pqkl,lb->pqab', cosines, retained, cosines, precision=precise)
        return ((renewed - from_spans(restored)).astype(jnp.bfloat16), picked.astype(jnp.bfloat16))
    new_momentum, values = lax.map(compress, (gradient, momentum, indices))

    def absorb(running, operands):
        shipped, chosen = operands
        return (running.at[block_rows, block_cols, chosen].add(shipped.astype(jnp.float32)), None)
    start_sum = jnp.zeros((row_blocks, col_blocks, BLOCK * BLOCK), jnp.float32)
    combined, unused = lax.scan(absorb, start_sum, (values, indices))
    combined = combined.reshape(row_blocks, col_blocks, BLOCK, BLOCK)
    decoded = from_spans(jnp.einsum('ka,pqkl,lb->pqab', cosines, combined, cosines, precision=precise))
    spread = jnp.sqrt(jnp.mean(decoded * decoded) + EPSILON)
    update = (decoded / spread).astype(jnp.bfloat16)
    return (new_momentum, update)
```

```python
import functools

import jax
import jax.numpy as jnp
import numpy as np
from jax import lax
from jax.experimental import pallas as pl
from jax.experimental.pallas import tpu as pltpu
from jax.sharding import PartitionSpec as P

BLOCK = 64
LANES = 128
SUBLANES = 8
EPSILON = 1e-06
DECAY = 0.999
F32 = jnp.float32
BF16 = jnp.bfloat16
MESH = pl.DeviceIdType.MESH


def dct_basis(edge):
    frequency = np.arange(edge, dtype=np.float64)[:, None]
    position = np.arange(edge, dtype=np.float64)[None, :]
    waves = np.cos(np.pi * (2.0 * position + 1.0) * frequency / (2.0 * edge))
    weights = np.where(frequency == 0.0, np.sqrt(1.0 / edge), np.sqrt(2.0 / edge))
    return (waves * weights).astype(np.float32)


def halves(x):
    high = x.astype(BF16)
    return high, (x - high.astype(F32)).astype(BF16)


def np_halves(x):
    high = x.astype(jnp.bfloat16)
    return high, (x - high.astype(np.float32)).astype(jnp.bfloat16)


def dot(a, b):
    return jnp.dot(a, b, preferred_element_type=F32)


def dot_nt(a, b):
    return lax.dot_general(a, b, (((1,), (1,)), ((), ())), preferred_element_type=F32)


def wide(blocks, weights):
    tiles = [block[:, n * LANES:(n + 1) * LANES] for block in blocks for n in range(2)]
    high, low = halves(jnp.concatenate(tiles, axis=0))
    both = dot(jnp.concatenate([high, low], axis=1), weights)
    out = both[:, :LANES] + both[:, LANES:]
    parts = [out[n * BLOCK:(n + 1) * BLOCK] for n in range(len(tiles))]
    return [jnp.concatenate(parts[2 * n:2 * n + 2], axis=1) for n in range(len(blocks))]


def kernel(
    replicas, shards,
    grad_hbm, mom_hbm, idx_hbm, fwd_hbm, inv_hbm, deep_hbm, rows_hbm,
    newm_ref, dense_ref, e_in,
    grad, mom, idx, fwd, inv, deep, rows,
    by_span, picks, high_even, low_even, high_odd, low_odd, factor,
    ids, all_ids, shipped, all_values, span_a, span_b, span_v, mixed_even, mixed_odd, e_out,
    x_sem, c_sem, id_sem, value_sem, e_send, e_recv,
):
    me = lax.axis_index("dp")
    part = lax.axis_index("tensor")
    barrier = pltpu.get_barrier_semaphore()

    topk, spans = idx.shape
    fold = LANES // topk
    width = fold * BLOCK
    groups = spans // fold
    chunks = groups // SUBLANES
    stretch = SUBLANES * width
    depth = replicas * topk

    loads = [pltpu.make_async_copy(src, dst, c_sem.at[n]) for n, (src, dst) in enumerate(
        [(idx_hbm, idx), (fwd_hbm, fwd), (rows_hbm, rows), (inv_hbm, inv), (deep_hbm, deep)])]

    def slab(c):
        cols = pl.ds(c * stretch, stretch)
        return [pltpu.make_async_copy(src.at[:, cols], dst.at[:, cols], x_sem.at[n, c])
                for n, (src, dst) in enumerate([(mom_hbm, mom), (grad_hbm, grad)])]

    loads[0].start()
    loads[1].start()
    for copy in slab(0):
        copy.start()
    loads[2].start()
    for c in range(1, chunks):
        for copy in slab(c):
            copy.start()
    loads[3].start()
    loads[4].start()

    def greet_dp(k, c):
        pl.semaphore_signal(barrier, inc=1, device_id={"dp": lax.rem(me + k, replicas)}, device_id_type=MESH)
        return c

    def greet_tp(k, c):
        pl.semaphore_signal(barrier, inc=1, device_id={"tensor": lax.rem(part + k, shards)}, device_id_type=MESH)
        return c

    lax.fori_loop(1, replicas, greet_dp, 0)
    lax.fori_loop(1, shards, greet_tp, 0)

    loads[0].wait()
    by_span[...] = idx[...].T
    chosen = jnp.concatenate(
        [by_span[pl.ds(s, groups, stride=fold), :] for s in range(fold)], axis=1
    )
    ids[...] = chosen.astype(jnp.int16)
    picks[0] = (chosen // BLOCK).astype(F32)
    slot = lax.broadcasted_iota(jnp.int32, chosen.shape, 1) // topk
    picks[1] = (chosen % BLOCK + BLOCK * slot).astype(F32)

    zero = jnp.zeros((), BF16)
    one = jnp.ones((), BF16)
    tall = lax.broadcasted_iota(jnp.int32, (width, LANES), 0).astype(F32).astype(BF16)
    short = lax.broadcasted_iota(jnp.int32, (BLOCK, LANES), 0).astype(F32).astype(BF16)
    level = lax.broadcasted_iota(jnp.int32, (BLOCK, depth), 0).astype(F32).astype(BF16)

    def hot(levels, plane, g):
        return jnp.where(levels == picks[plane, pl.ds(g, 1), :].astype(BF16), one, zero)

    def columns(g, size):
        return pl.ds(g * size, size)

    def members(c):
        return range(c * SUBLANES, (c + 1) * SUBLANES)

    def renew(g):
        cols = columns(g, width)
        return DECAY * mom[:, cols].astype(F32) + grad[:, cols].astype(F32)

    highs, lows = (high_even, high_odd), (low_even, low_odd)

    def transform(c):
        high, low = highs[c % 2], lows[c % 2]
        for u, block in enumerate(wide([renew(g) for g in members(c)], fwd[...])):
            high[u], low[u] = halves(block)

    def pick(c):
        high, low = highs[c % 2], lows[c % 2]
        found = []
        for u, g in enumerate(members(c)):
            both = dot(jnp.concatenate([high[u], low[u]], axis=0), hot(tall, 1, g))
            row_hot = hot(short, 0, g)
            waves = dot(rows[...], jnp.concatenate([row_hot, row_hot], axis=0))
            value = jnp.sum((both[:BLOCK] + both[BLOCK:]) * waves, axis=0, keepdims=True)
            found.append(value)
            factor[:, columns(g, 2 * LANES)] = jnp.concatenate(halves(waves * value), axis=1)
        shipped[c] = jnp.concatenate(found, axis=0).astype(BF16)

    def restore(c):
        spread = []
        for g in members(c):
            col_hot = hot(tall, 1, g)
            spread.append(dot_nt(factor[:, columns(g, 2 * LANES)], jnp.concatenate([col_hot, col_hot], axis=1)))
        for g, block in zip(members(c), wide(spread, inv[...])):
            newm_ref[:, columns(g, width)] = (renew(g) - block).astype(BF16)

    def id_copy(k, slot):
        return pltpu.make_async_remote_copy(
            src_ref=ids, dst_ref=all_ids.at[slot],
            send_sem=id_sem.at[0, k], recv_sem=id_sem.at[1, k],
            device_id={"dp": lax.rem(me + k, replicas)}, device_id_type=MESH,
        )

    def value_copy(c, k, slot):
        return pltpu.make_async_remote_copy(
            src_ref=shipped.at[c], dst_ref=all_values.at[c, slot],
            send_sem=value_sem.at[c, 0, k], recv_sem=value_sem.at[c, 1, k],
            device_id={"dp": lax.rem(me + k, replicas)}, device_id_type=MESH,
        )

    def each(act):
        def step(k, c):
            act(k)
            return c
        lax.fori_loop(1, replicas, step, 0)

    def source(k):
        return lax.rem(me - k + replicas, replicas)

    def ship(c):
        each(lambda k: value_copy(c, k, me).start())
        all_values[c, me] = shipped[c]

    loads[1].wait()
    for copy in slab(0):
        copy.wait()
    transform(0)
    loads[2].wait()
    for c in range(chunks):
        if c + 1 < chunks:
            for copy in slab(c + 1):
                copy.wait()
            transform(c + 1)
        pick(c)
        if c == 0:
            pl.semaphore_wait(barrier, replicas - 1 + shards - 1)
            each(lambda k: id_copy(k, me).start())
            all_ids[me] = ids[...]
        ship(c)

    loads[3].wait()
    loads[4].wait()
    for c in range(chunks):
        restore(c)

    each(lambda k: id_copy(k, source(k)).wait_recv())
    for s in range(fold):
        lines = slice(s * groups, (s + 1) * groups)
        lanes = slice(s * topk, (s + 1) * topk)
        named = jnp.concatenate([all_ids[r].astype(jnp.int32)[:, lanes] for r in range(replicas)], axis=1)
        span_a[lines, :] = (named // BLOCK).astype(F32)
        span_b[lines, :] = (named % BLOCK).astype(F32)

    mixes = (mixed_even, mixed_odd)

    def densify(c, energy):
        mixed = mixes[c % 2]
        tiles = []
        for s in range(fold):
            lanes = slice(s * topk, (s + 1) * topk)
            lines = pl.ds(s * groups + c * SUBLANES, SUBLANES)
            span_v[s] = jnp.concatenate([all_values[c, r].astype(F32)[:, lanes] for r in range(replicas)], axis=1)
            tiles.append((span_a[lines, :], span_b[lines, :], span_v[s]))
        for u in range(SUBLANES):
            blocks = []
            for s in range(fold):
                a, b, v = (tile[u:u + 1].astype(BF16) for tile in tiles[s])
                row_hot = jnp.where(level == a, v, zero)
                col_hot = jnp.where(level == b, one, zero)
                blocks.append(dot_nt(row_hot, col_hot))
            combined = jnp.concatenate(blocks, axis=1)
            mixed[u] = combined.astype(BF16)
            energy = energy + jnp.sum((combined * combined).reshape(BLOCK // SUBLANES, SUBLANES, width), axis=0)
        return energy

    def decode(c):
        mixed = mixes[c % 2]
        tall_mix = jnp.concatenate([mixed[u] for u in range(SUBLANES)], axis=0)
        across = dot(jnp.concatenate([tall_mix, tall_mix], axis=1), deep[...]).astype(BF16)
        for u, g in enumerate(members(c)):
            block = across[u * BLOCK:(u + 1) * BLOCK]
            dense_ref[:, columns(g, width)] = dot(rows[...], jnp.concatenate([block, block], axis=0))

    energy = jnp.zeros((SUBLANES, width), F32)
    for c in range(chunks):
        each(lambda k: value_copy(c, k, source(k)).wait_recv())
        energy = densify(c, energy)
        if c:
            decode(c - 1)

    energy = sum(energy[:, n * LANES:(n + 1) * LANES] for n in range(width // LANES))
    e_out[...] = energy
    e_in[part] = energy

    def copy_tp(k, slot):
        return pltpu.make_async_remote_copy(
            src_ref=e_out, dst_ref=e_in.at[slot],
            send_sem=e_send.at[k], recv_sem=e_recv.at[k],
            device_id={"tensor": lax.rem(part + k, shards)}, device_id_type=MESH,
        )

    def start_tp(k, c):
        copy_tp(k, part).start()
        return c

    def finish_tp(k, c):
        copy_tp(k, lax.rem(part - k + shards, shards)).wait()
        return c

    lax.fori_loop(1, shards, start_tp, 0)
    decode(chunks - 1)
    each(lambda k: id_copy(k, me).wait_send())
    for c in range(chunks):
        each(lambda k: value_copy(c, k, me).wait_send())
    lax.fori_loop(1, shards, finish_tp, 0)


def finish(total, newm_ref, dense_ref, e_ref, newm_hbm, upd_hbm, upd, sems):
    first = pltpu.make_async_copy(newm_ref, newm_hbm, sems.at[0])
    first.start()
    pieces = sems.shape[0] - 1
    stretch = upd.shape[1] // pieces
    mean = jnp.sum(e_ref[...]) / total
    scale = lax.rsqrt(jnp.full((1, stretch), mean + EPSILON, F32))
    copies = []
    for n in range(pieces):
        cols = pl.ds(n * stretch, stretch)
        upd[:, cols] = (dense_ref[:, cols] * scale).astype(BF16)
        copies.append(pltpu.make_async_copy(upd.at[:, cols], upd_hbm.at[:, cols], sems.at[n + 1]))
        copies[-1].start()
    first.wait()
    for copy in copies:
        copy.wait()


def local(gradient, momentum, indices, replicas, shards):
    height, cols = gradient.shape[1:]
    topk = indices.shape[-1]
    fold = LANES // topk
    spans = cols // BLOCK
    groups = spans // fold
    width = fold * BLOCK
    chunks = groups // SUBLANES
    assert height == BLOCK and chunks * SUBLANES * fold == spans and width == 2 * LANES
    basis = dct_basis(BLOCK)
    pair = np.eye(2, dtype=np.float32)
    both = [np.concatenate(np_halves(np.kron(pair, w)), axis=1) for w in (basis.T, basis)]
    fwd, inv = (jnp.asarray(np.concatenate([w, w], axis=0)) for w in both)
    deep = jnp.asarray(np.concatenate(np_halves(np.kron(np.eye(fold, dtype=np.float32), basis)), axis=0))
    rows = jnp.asarray(np.concatenate(np_halves(basis.T), axis=1))
    depth = max(replicas * topk, LANES)
    vmem = pl.BlockSpec(memory_space=pltpu.VMEM)
    hbm = pl.BlockSpec(memory_space=pltpu.HBM)
    half = pltpu.VMEM((SUBLANES, height, width), BF16)
    operands = (gradient[0], momentum[0], indices.reshape(spans, topk).T, fwd, inv, deep, rows)
    newm, dense, energy = pl.pallas_call(
        functools.partial(kernel, replicas, shards),
        out_shape=(
            jax.ShapeDtypeStruct((height, cols), BF16),
            jax.ShapeDtypeStruct((height, cols), F32),
            jax.ShapeDtypeStruct((shards, SUBLANES, LANES), F32),
        ),
        in_specs=[hbm] * 7,
        out_specs=(vmem, vmem, vmem),
        scratch_shapes=[
            pltpu.VMEM((height, cols), BF16),
            pltpu.VMEM((height, cols), BF16),
            pltpu.VMEM((topk, spans), jnp.int32),
            pltpu.VMEM(fwd.shape, BF16),
            pltpu.VMEM(inv.shape, BF16),
            pltpu.VMEM(deep.shape, BF16),
            pltpu.VMEM(rows.shape, BF16),
            pltpu.VMEM((spans, topk), jnp.int32),
            pltpu.VMEM((2, groups, LANES), F32),
            half, half, half, half,
            pltpu.VMEM((height, groups * 2 * LANES), BF16),
            pltpu.VMEM((groups, LANES), jnp.int16),
            pltpu.VMEM((replicas, groups, LANES), jnp.int16),
            pltpu.VMEM((chunks, SUBLANES, LANES), BF16),
            pltpu.VMEM((chunks, replicas, SUBLANES, LANES), BF16),
            pltpu.VMEM((spans, depth), F32),
            pltpu.VMEM((spans, depth), F32),
            pltpu.VMEM((fold, SUBLANES, depth), F32),
            half, half,
            pltpu.VMEM((SUBLANES, LANES), F32),
            pltpu.SemaphoreType.DMA((2, chunks)),
            pltpu.SemaphoreType.DMA((5,)),
            pltpu.SemaphoreType.DMA((2, replicas)),
            pltpu.SemaphoreType.DMA((chunks, 2, replicas)),
            pltpu.SemaphoreType.DMA((shards,)),
            pltpu.SemaphoreType.DMA((shards,)),
        ],
        compiler_params=pltpu.CompilerParams(
            collective_id=0, has_side_effects=True, vmem_limit_bytes=24 * 2 ** 20
        ),
        name="demo_step",
    )(*(pltpu.with_memory_space_constraint(x, pltpu.HBM) for x in operands))
    newm, update = pl.pallas_call(
        functools.partial(finish, float(height * cols * shards)),
        out_shape=(
            jax.ShapeDtypeStruct((height, cols), BF16),
            jax.ShapeDtypeStruct((height, cols), BF16),
        ),
        in_specs=[vmem] * 3,
        out_specs=(hbm, hbm),
        scratch_shapes=[pltpu.VMEM((height, cols), BF16), pltpu.SemaphoreType.DMA((5,))],
        compiler_params=pltpu.CompilerParams(vmem_limit_bytes=8 * 2 ** 20),
        name="finish",
    )(newm, dense, energy)
    return newm[None], update


def solution(mesh):
    in_specs = (P("dp", "tensor", None), P("dp", "tensor", None), P("dp", "tensor", None, None))
    out_specs = (P("dp", "tensor", None), P("tensor", None))
    body = functools.partial(local, replicas=mesh.shape["dp"], shards=mesh.shape["tensor"])
    return jax.shard_map(body, mesh=mesh, in_specs=in_specs, out_specs=out_specs, check_vma=False)
```

```python
import functools

import jax
import jax.numpy as jnp
import numpy as np
from jax import lax
from jax.experimental import pallas as pl
from jax.experimental.pallas import tpu as pltpu
from jax.sharding import PartitionSpec as P

BLOCK = 64
LANES = 128
SUBLANES = 8
EPSILON = 1e-06
DECAY = 0.999
F32 = jnp.float32
BF16 = jnp.bfloat16
MESH = pl.DeviceIdType.MESH


def dct_basis(edge):
    frequency = np.arange(edge, dtype=np.float64)[:, None]
    position = np.arange(edge, dtype=np.float64)[None, :]
    waves = np.cos(np.pi * (2.0 * position + 1.0) * frequency / (2.0 * edge))
    weights = np.where(frequency == 0.0, np.sqrt(1.0 / edge), np.sqrt(2.0 / edge))
    return (waves * weights).astype(np.float32)


def halves(x):
    high = x.astype(BF16)
    return high, (x - high.astype(F32)).astype(BF16)


def np_halves(x):
    high = x.astype(jnp.bfloat16)
    return high, (x - high.astype(np.float32)).astype(jnp.bfloat16)


def dot(a, b):
    return jnp.dot(a, b, preferred_element_type=F32)


def dot_nt(a, b):
    return lax.dot_general(a, b, (((1,), (1,)), ((), ())), preferred_element_type=F32)


def wide(blocks, weights):
    tiles = [block[:, n * LANES:(n + 1) * LANES] for block in blocks for n in range(2)]
    high, low = halves(jnp.concatenate(tiles, axis=0))
    both = dot(jnp.concatenate([high, low], axis=1), weights)
    out = both[:, :LANES] + both[:, LANES:]
    parts = [out[n * BLOCK:(n + 1) * BLOCK] for n in range(len(tiles))]
    return [jnp.concatenate(parts[2 * n:2 * n + 2], axis=1) for n in range(len(blocks))]


def kernel(
    replicas, shards,
    grad_hbm, mom_hbm, idx_hbm, fwd_hbm, inv_hbm, deep_hbm, rows_hbm,
    newm_ref, dense_ref, e_in,
    grad, mom, idx, fwd, inv, deep, rows,
    by_span, picks, high_even, low_even, high_odd, low_odd, factor,
    ids, all_ids, values, shipped, all_values, span_a, span_b, span_v, partial, mixed, e_out,
    x_sem, c_sem, id_sem, value_sem, id_in, value_in, ready, e_send, e_recv,
):
    me = lax.axis_index("dp")
    part = lax.axis_index("tensor")
    barrier = pltpu.get_barrier_semaphore()

    topk, spans = idx.shape
    fold = LANES // topk
    width = fold * BLOCK
    groups = spans // fold
    chunks = groups // SUBLANES
    stretch = SUBLANES * width
    team = all_ids.shape[1]
    teams = replicas // team
    depth = team * topk
    home = me // team

    loads = [pltpu.make_async_copy(src, dst, c_sem.at[n]) for n, (src, dst) in enumerate(
        [(idx_hbm, idx), (fwd_hbm, fwd), (rows_hbm, rows), (inv_hbm, inv), (deep_hbm, deep)])]

    def slab(c):
        cols = pl.ds(c * stretch, stretch)
        return [pltpu.make_async_copy(src.at[:, cols], dst.at[:, cols], x_sem.at[n, c])
                for n, (src, dst) in enumerate([(mom_hbm, mom), (grad_hbm, grad)])]

    loads[0].start()
    loads[1].start()
    for copy in slab(0):
        copy.start()
    loads[2].start()
    for c in range(1, chunks):
        for copy in slab(c):
            copy.start()
    loads[3].start()
    loads[4].start()

    def each(low, high, act):
        def step(k, c):
            act(k)
            return c
        lax.fori_loop(low, high, step, 0)

    def peer(j):
        return dict(device_id={"dp": j}, device_id_type=MESH)

    def mate(k):
        return dict(device_id={"tensor": lax.rem(part + k, shards)}, device_id_type=MESH)

    each(me + 1, replicas, lambda j: pl.semaphore_signal(barrier, inc=1, **peer(j)))
    each(1, shards, lambda k: pl.semaphore_signal(barrier, inc=1, **mate(k)))
    pl.semaphore_wait(barrier, me + shards - 1)
    each(0, me, lambda j: pl.semaphore_signal(ready.at[me], inc=1, **peer(j)))

    loads[0].wait()
    by_span[...] = idx[...].T
    chosen = jnp.concatenate(
        [by_span[pl.ds(s, groups, stride=fold), :] for s in range(fold)], axis=1
    )
    ids[...] = chosen.astype(jnp.int16)
    picks[0] = (chosen // BLOCK).astype(F32)
    slot = lax.broadcasted_iota(jnp.int32, chosen.shape, 1) // topk
    picks[1] = (chosen % BLOCK + BLOCK * slot).astype(F32)

    zero = jnp.zeros((), BF16)
    one = jnp.ones((), BF16)
    tall = lax.broadcasted_iota(jnp.int32, (width, LANES), 0).astype(F32).astype(BF16)
    short = lax.broadcasted_iota(jnp.int32, (BLOCK, LANES), 0).astype(F32).astype(BF16)
    level = lax.broadcasted_iota(jnp.int32, (BLOCK, depth), 0).astype(F32).astype(BF16)

    def hot(levels, plane, g):
        return jnp.where(levels == picks[plane, pl.ds(g, 1), :].astype(BF16), one, zero)

    def columns(g, size):
        return pl.ds(g * size, size)

    def members(c):
        return range(c * SUBLANES, (c + 1) * SUBLANES)

    def renew(g):
        cols = columns(g, width)
        return DECAY * mom[:, cols].astype(F32) + grad[:, cols].astype(F32)

    highs, lows = (high_even, high_odd), (low_even, low_odd)

    def transform(c):
        high, low = highs[c % 2], lows[c % 2]
        for u, block in enumerate(wide([renew(g) for g in members(c)], fwd[...])):
            high[u], low[u] = halves(block)

    def pick(c):
        high, low = highs[c % 2], lows[c % 2]
        for u, g in enumerate(members(c)):
            both = dot(jnp.concatenate([high[u], low[u]], axis=0), hot(tall, 1, g))
            row_hot = hot(short, 0, g)
            waves = dot(rows[...], jnp.concatenate([row_hot, row_hot], axis=0))
            value = jnp.sum((both[:BLOCK] + both[BLOCK:]) * waves, axis=0, keepdims=True)
            values[pl.ds(g, 1), :] = value
            factor[:, columns(g, 2 * LANES)] = jnp.concatenate(halves(waves * value), axis=1)

    def restore(c):
        spread = []
        for g in members(c):
            col_hot = hot(tall, 1, g)
            spread.append(dot_nt(factor[:, columns(g, 2 * LANES)], jnp.concatenate([col_hot, col_hot], axis=1)))
        for g, block in zip(members(c), wide(spread, inv[...])):
            newm_ref[:, columns(g, width)] = (renew(g) - block).astype(BF16)

    def copies(src, dst, sends, arrivals, j):
        return pltpu.make_async_remote_copy(
            src_ref=src, dst_ref=dst.at[home, lax.rem(me, team)],
            send_sem=sends.at[0], recv_sem=arrivals.at[home], **peer(j),
        )

    def send_ids(j):
        copies(ids, all_ids, id_sem, id_in, j).start()

    def send_values(j):
        copies(shipped, all_values, value_sem, value_in, j).start()

    def greet(j):
        pl.semaphore_wait(ready.at[j], 1)
        send_ids(j)
        send_values(j)

    def bulk(dst, sends, arrivals, t, count):
        ref = dst.at[t, pl.ds(0, count)]
        return pltpu.make_async_remote_copy(
            src_ref=ref, dst_ref=ref, send_sem=sends.at[0], recv_sem=arrivals.at[t], **peer(me),
        )

    each(0, me, send_ids)
    all_ids[home, lax.rem(me, team)] = ids[...]

    loads[1].wait()
    for copy in slab(0):
        copy.wait()
    transform(0)
    loads[2].wait()
    for c in range(chunks):
        if c + 1 < chunks:
            for copy in slab(c + 1):
                copy.wait()
            transform(c + 1)
        pick(c)
    shipped[...] = values[...].astype(BF16)
    each(0, me, send_values)
    all_values[home, lax.rem(me, team)] = shipped[...]

    loads[3].wait()
    restore(0)
    each(me + 1, (home + 1) * team, greet)
    for c in range(1, chunks):
        restore(c)
    each((home + 1) * team, replicas, greet)
    loads[4].wait()

    def name(n, t):
        for s in range(fold):
            lines = slice(s * groups, (s + 1) * groups)
            lanes = slice(s * topk, (s + 1) * topk)
            named = jnp.concatenate([all_ids[t, r].astype(jnp.int32)[:, lanes] for r in range(team)], axis=1)
            span_a[n, lines, :] = (named // BLOCK).astype(F32)
            span_b[n, lines, :] = (named % BLOCK).astype(F32)

    def gather(n, t):
        for s in range(fold):
            lines = slice(s * groups, (s + 1) * groups)
            lanes = slice(s * topk, (s + 1) * topk)
            span_v[n, lines, :] = jnp.concatenate([all_values[t, r].astype(F32)[:, lanes] for r in range(team)], axis=1)

    def densify(n, c, energy):
        tiles = []
        for s in range(fold):
            lines = pl.ds(s * groups + c * SUBLANES, SUBLANES)
            tiles.append([ref[n, lines, :] for ref in (span_a, span_b, span_v)])
        for u, g in enumerate(members(c)):
            blocks = []
            for s in range(fold):
                a, b, v = (tile[u:u + 1].astype(BF16) for tile in tiles[s])
                row_hot = jnp.where(level == a, v, zero)
                col_hot = jnp.where(level == b, one, zero)
                block = dot_nt(row_hot, col_hot)
                if n:
                    block = block + partial[g * fold + s]
                if n + 1 < teams:
                    partial[g * fold + s] = block
                blocks.append(block)
            if n + 1 == teams:
                combined = jnp.concatenate(blocks, axis=1)
                mixed[g] = combined.astype(BF16)
                energy = energy + jnp.sum((combined * combined).reshape(BLOCK // SUBLANES, SUBLANES, width), axis=0)
        return energy

    def decode(c):
        stack = jnp.concatenate([mixed[g] for g in members(c)], axis=0)
        across = dot(jnp.concatenate([stack, stack], axis=1), deep[...]).astype(BF16)
        for u, g in enumerate(members(c)):
            block = across[u * BLOCK:(u + 1) * BLOCK]
            dense_ref[:, columns(g, width)] = dot(rows[...], jnp.concatenate([block, block], axis=0))

    energy = jnp.zeros((SUBLANES, width), F32)
    for n in range(teams):
        t = lax.rem(home + n, teams)
        count = team if n else team - 1
        bulk(all_ids, id_sem, id_in, t, count).wait_recv()
        name(n, t)
        bulk(all_values, value_sem, value_in, t, count).wait_recv()
        gather(n, t)
        for c in range(chunks):
            energy = densify(n, c, energy)

    energy = sum(energy[:, n * LANES:(n + 1) * LANES] for n in range(width // LANES))
    e_out[...] = energy
    e_in[part] = energy

    def copy_tp(k, slot):
        return pltpu.make_async_remote_copy(
            src_ref=e_out, dst_ref=e_in.at[slot],
            send_sem=e_send.at[k], recv_sem=e_recv.at[k], **mate(k),
        )

    each(1, shards, lambda k: copy_tp(k, part).start())
    for c in range(chunks):
        decode(c)
    for dst, sends, arrivals in ((all_ids, id_sem, id_in), (all_values, value_sem, value_in)):
        for n in range(teams):
            bulk(dst, sends, arrivals, n, team if n else team - 1).wait_send()
    each(1, shards, lambda k: copy_tp(k, lax.rem(part - k + shards, shards)).wait())


def finish(total, newm_ref, dense_ref, e_ref, newm_hbm, upd_hbm, upd, sems):
    first = pltpu.make_async_copy(newm_ref, newm_hbm, sems.at[0])
    first.start()
    pieces = sems.shape[0] - 1
    stretch = upd.shape[1] // pieces
    mean = jnp.sum(e_ref[...]) / total
    scale = lax.rsqrt(jnp.full((1, stretch), mean + EPSILON, F32))
    copies = []
    for n in range(pieces):
        cols = pl.ds(n * stretch, stretch)
        upd[:, cols] = (dense_ref[:, cols] * scale).astype(BF16)
        copies.append(pltpu.make_async_copy(upd.at[:, cols], upd_hbm.at[:, cols], sems.at[n + 1]))
        copies[-1].start()
    first.wait()
    for copy in copies:
        copy.wait()


def local(gradient, momentum, indices, replicas, shards):
    height, cols = gradient.shape[1:]
    topk = indices.shape[-1]
    fold = LANES // topk
    spans = cols // BLOCK
    groups = spans // fold
    width = fold * BLOCK
    chunks = groups // SUBLANES
    assert height == BLOCK and chunks * SUBLANES * fold == spans and width == 2 * LANES
    basis = dct_basis(BLOCK)
    pair = np.eye(2, dtype=np.float32)
    both = [np.concatenate(np_halves(np.kron(pair, w)), axis=1) for w in (basis.T, basis)]
    fwd, inv = (jnp.asarray(np.concatenate([w, w], axis=0)) for w in both)
    deep = jnp.asarray(np.concatenate(np_halves(np.kron(np.eye(fold, dtype=np.float32), basis)), axis=0))
    rows = jnp.asarray(np.concatenate(np_halves(basis.T), axis=1))
    team = min(replicas, 2 * LANES // topk)
    teams = replicas // team
    depth = team * topk
    assert teams * team == replicas and depth % LANES == 0
    vmem = pl.BlockSpec(memory_space=pltpu.VMEM)
    hbm = pl.BlockSpec(memory_space=pltpu.HBM)
    half = pltpu.VMEM((SUBLANES, height, width), BF16)
    operands = (gradient[0], momentum[0], indices.reshape(spans, topk).T, fwd, inv, deep, rows)
    newm, dense, energy = pl.pallas_call(
        functools.partial(kernel, replicas, shards),
        out_shape=(
            jax.ShapeDtypeStruct((height, cols), BF16),
            jax.ShapeDtypeStruct((height, cols), F32),
            jax.ShapeDtypeStruct((shards, SUBLANES, LANES), F32),
        ),
        in_specs=[hbm] * 7,
        out_specs=(vmem, vmem, vmem),
        scratch_shapes=[
            pltpu.VMEM((height, cols), BF16),
            pltpu.VMEM((height, cols), BF16),
            pltpu.VMEM((topk, spans), jnp.int32),
            pltpu.VMEM(fwd.shape, BF16),
            pltpu.VMEM(inv.shape, BF16),
            pltpu.VMEM(deep.shape, BF16),
            pltpu.VMEM(rows.shape, BF16),
            pltpu.VMEM((spans, topk), jnp.int32),
            pltpu.VMEM((2, groups, LANES), F32),
            half, half, half, half,
            pltpu.VMEM((height, groups * 2 * LANES), BF16),
            pltpu.VMEM((groups, LANES), jnp.int16),
            pltpu.VMEM((teams, team, groups, LANES), jnp.int16),
            pltpu.VMEM((groups, LANES), F32),
            pltpu.VMEM((groups, LANES), BF16),
            pltpu.VMEM((teams, team, groups, LANES), BF16),
            pltpu.VMEM((teams, spans, depth), F32),
            pltpu.VMEM((teams, spans, depth), F32),
            pltpu.VMEM((teams, spans, depth), F32),
            pltpu.VMEM((spans, height, BLOCK), F32),
            pltpu.VMEM((groups, height, width), BF16),
            pltpu.VMEM((SUBLANES, LANES), F32),
            pltpu.SemaphoreType.DMA((2, chunks)),
            pltpu.SemaphoreType.DMA((5,)),
            pltpu.SemaphoreType.DMA((1,)),
            pltpu.SemaphoreType.DMA((1,)),
            pltpu.SemaphoreType.DMA((teams,)),
            pltpu.SemaphoreType.DMA((teams,)),
            pltpu.SemaphoreType.REGULAR((replicas,)),
            pltpu.SemaphoreType.DMA((shards,)),
            pltpu.SemaphoreType.DMA((shards,)),
        ],
        compiler_params=pltpu.CompilerParams(
            collective_id=0, has_side_effects=True, vmem_limit_bytes=24 * 2 ** 20
        ),
        name="demo_step",
    )(*(pltpu.with_memory_space_constraint(x, pltpu.HBM) for x in operands))
    newm, update = pl.pallas_call(
        functools.partial(finish, float(height * cols * shards)),
        out_shape=(
            jax.ShapeDtypeStruct((height, cols), BF16),
            jax.ShapeDtypeStruct((height, cols), BF16),
        ),
        in_specs=[vmem] * 3,
        out_specs=(hbm, hbm),
        scratch_shapes=[pltpu.VMEM((height, cols), BF16), pltpu.SemaphoreType.DMA((5,))],
        compiler_params=pltpu.CompilerParams(vmem_limit_bytes=8 * 2 ** 20),
        name="finish",
    )(newm, dense, energy)
    return newm[None], update


def solution(mesh):
    in_specs = (P("dp", "tensor", None), P("dp", "tensor", None), P("dp", "tensor", None, None))
    out_specs = (P("dp", "tensor", None), P("tensor", None))
    body = functools.partial(local, replicas=mesh.shape["dp"], shards=mesh.shape["tensor"])
    return jax.shard_map(body, mesh=mesh, in_specs=in_specs, out_specs=out_specs, check_vma=False)
```

```python
import functools

import jax
import jax.numpy as jnp
import numpy as np
from jax import lax
from jax.experimental import pallas as pl
from jax.experimental.pallas import tpu as pltpu
from jax.sharding import PartitionSpec as P

BLOCK = 64
LANES = 128
SUBLANES = 8
EPSILON = 1e-06
DECAY = 0.999
F32 = jnp.float32
BF16 = jnp.bfloat16
MESH = pl.DeviceIdType.MESH


def dct_basis(edge):
    frequency = np.arange(edge, dtype=np.float64)[:, None]
    position = np.arange(edge, dtype=np.float64)[None, :]
    waves = np.cos(np.pi * (2.0 * position + 1.0) * frequency / (2.0 * edge))
    weights = np.where(frequency == 0.0, np.sqrt(1.0 / edge), np.sqrt(2.0 / edge))
    return (waves * weights).astype(np.float32)


def halves(x):
    high = x.astype(BF16)
    return high, (x - high.astype(F32)).astype(BF16)


def np_halves(x):
    high = x.astype(jnp.bfloat16)
    return high, (x - high.astype(np.float32)).astype(jnp.bfloat16)


def dot(a, b):
    return jnp.dot(a, b, preferred_element_type=F32)


def dot_nt(a, b):
    return lax.dot_general(a, b, (((1,), (1,)), ((), ())), preferred_element_type=F32)


def wide(blocks, weights):
    tiles = [block[:, n * LANES:(n + 1) * LANES] for block in blocks for n in range(2)]
    high, low = halves(jnp.concatenate(tiles, axis=0))
    both = dot(jnp.concatenate([high, low], axis=1), weights)
    out = both[:, :LANES] + both[:, LANES:]
    parts = [out[n * BLOCK:(n + 1) * BLOCK] for n in range(len(tiles))]
    return [jnp.concatenate(parts[2 * n:2 * n + 2], axis=1) for n in range(len(blocks))]


def decode(blocks, deep, rows):
    stack = jnp.concatenate(blocks, axis=0)
    across = dot(jnp.concatenate([stack, stack], axis=1), deep).astype(BF16)
    parts = [across[u * BLOCK:(u + 1) * BLOCK] for u in range(len(blocks))]
    return [dot(rows, jnp.concatenate([part, part], axis=0)) for part in parts]


def kernel(
    replicas, shards,
    grad_hbm, mom_hbm, idx_hbm, fwd_hbm, inv_hbm, deep_hbm, rows_hbm,
    newm_ref, dense_ref, e_in, last_ref, deep_ref, basis_ref,
    grad, mom, idx, fwd, inv, deep, rows,
    by_span, picks, high_even, low_even, high_odd, low_odd, factor,
    ids, all_ids, values, shipped, all_values, span_a, span_b, span_v, partial, mixed, e_out,
    x_sem, c_sem, id_sem, value_sem, id_in, value_in, ready, e_send, e_recv,
):
    me = lax.axis_index("dp")
    part = lax.axis_index("tensor")
    barrier = pltpu.get_barrier_semaphore()

    topk, spans = idx.shape
    fold = LANES // topk
    width = fold * BLOCK
    groups = spans // fold
    chunks = groups // SUBLANES
    stretch = SUBLANES * width
    team = all_ids.shape[1]
    teams = replicas // team
    depth = team * topk
    home = me // team
    parts, half = shipped.shape[:2]
    own = lax.rem(me, team)

    loads = [pltpu.make_async_copy(src, dst, c_sem.at[n]) for n, (src, dst) in enumerate(
        [(idx_hbm, idx), (fwd_hbm, fwd), (rows_hbm, rows), (inv_hbm, inv), (deep_hbm, deep)])]

    def slab(c):
        cols = pl.ds(c * stretch, stretch)
        return [pltpu.make_async_copy(src.at[:, cols], dst.at[:, cols], x_sem.at[n, c])
                for n, (src, dst) in enumerate([(mom_hbm, mom), (grad_hbm, grad)])]

    loads[0].start()
    loads[1].start()
    for copy in slab(0):
        copy.start()
    loads[2].start()
    for c in range(1, chunks):
        for copy in slab(c):
            copy.start()
    loads[3].start()
    loads[4].start()

    def each(low, high, act):
        def step(k, c):
            act(k)
            return c
        lax.fori_loop(low, high, step, 0)

    def peer(j):
        return dict(device_id={"dp": j}, device_id_type=MESH)

    def mate(k):
        return dict(device_id={"tensor": lax.rem(part + k, shards)}, device_id_type=MESH)

    each(me + 1, replicas, lambda j: pl.semaphore_signal(barrier, inc=1, **peer(j)))
    each(1, shards, lambda k: pl.semaphore_signal(barrier, inc=1, **mate(k)))
    pl.semaphore_wait(barrier, me + shards - 1)
    each(0, me, lambda j: pl.semaphore_signal(ready.at[me], inc=1, **peer(j)))

    loads[0].wait()
    by_span[...] = idx[...].T
    chosen = jnp.concatenate(
        [by_span[pl.ds(s, groups, stride=fold), :] for s in range(fold)], axis=1
    )
    ids[...] = chosen.astype(jnp.int16)
    picks[0] = (chosen // BLOCK).astype(F32)
    slot = lax.broadcasted_iota(jnp.int32, chosen.shape, 1) // topk
    picks[1] = (chosen % BLOCK + BLOCK * slot).astype(F32)

    zero = jnp.zeros((), BF16)
    one = jnp.ones((), BF16)
    tall = lax.broadcasted_iota(jnp.int32, (width, LANES), 0).astype(F32).astype(BF16)
    short = lax.broadcasted_iota(jnp.int32, (BLOCK, LANES), 0).astype(F32).astype(BF16)
    level = lax.broadcasted_iota(jnp.int32, (BLOCK, depth), 0).astype(F32).astype(BF16)

    def hot(levels, plane, g):
        return jnp.where(levels == picks[plane, pl.ds(g, 1), :].astype(BF16), one, zero)

    def columns(g, size):
        return pl.ds(g * size, size)

    def members(c):
        return range(c * SUBLANES, (c + 1) * SUBLANES)

    def renew(g):
        cols = columns(g, width)
        return DECAY * mom[:, cols].astype(F32) + grad[:, cols].astype(F32)

    highs, lows = (high_even, high_odd), (low_even, low_odd)

    def transform(c):
        high, low = highs[c % 2], lows[c % 2]
        for u, block in enumerate(wide([renew(g) for g in members(c)], fwd[...])):
            high[u], low[u] = halves(block)

    def pick(c):
        high, low = highs[c % 2], lows[c % 2]
        for u, g in enumerate(members(c)):
            both = dot(jnp.concatenate([high[u], low[u]], axis=0), hot(tall, 1, g))
            row_hot = hot(short, 0, g)
            waves = dot(rows[...], jnp.concatenate([row_hot, row_hot], axis=0))
            value = jnp.sum((both[:BLOCK] + both[BLOCK:]) * waves, axis=0, keepdims=True)
            values[pl.ds(g, 1), :] = value
            factor[:, columns(g, 2 * LANES)] = jnp.concatenate(halves(waves * value), axis=1)

    def restore(c):
        spread = []
        for g in members(c):
            col_hot = hot(tall, 1, g)
            spread.append(dot_nt(factor[:, columns(g, 2 * LANES)], jnp.concatenate([col_hot, col_hot], axis=1)))
        for g, block in zip(members(c), wide(spread, inv[...])):
            newm_ref[:, columns(g, width)] = (renew(g) - block).astype(BF16)

    def send(src, dst, send_sem, recv_sem, j):
        pltpu.make_async_remote_copy(
            src_ref=src, dst_ref=dst.at[home, own], send_sem=send_sem, recv_sem=recv_sem.at[home], **peer(j),
        ).start()

    def send_ids(j):
        send(ids, all_ids, id_sem.at[0], id_in, j)

    def send_values(p, j):
        send(shipped.at[p], all_values.at[p], value_sem.at[p], value_in.at[p], j)

    def keep(src, dst, sem):
        pltpu.make_async_copy(src, dst.at[home, own], sem.at[home]).start()

    def greet(j):
        pl.semaphore_wait(ready.at[j], 1)
        send_ids(j)
        for p in range(parts):
            send_values(p, j)

    def bulk(ref, send_sem, recv_sem):
        return pltpu.make_async_remote_copy(
            src_ref=ref, dst_ref=ref, send_sem=send_sem, recv_sem=recv_sem, **peer(me),
        )

    each(0, me, send_ids)
    keep(ids, all_ids, id_in)

    loads[1].wait()
    for copy in slab(0):
        copy.wait()
    transform(0)
    loads[2].wait()
    for c in range(chunks):
        if c + 1 < chunks:
            for copy in slab(c + 1):
                copy.wait()
            transform(c + 1)
        pick(c)
        p = (c + 1) * SUBLANES // half - 1
        if (c + 1) * SUBLANES == (p + 1) * half:
            shipped[p] = values[pl.ds(p * half, half), :].astype(BF16)
            each(0, me, functools.partial(send_values, p))
            keep(shipped.at[p], all_values.at[p], value_in.at[p])
    each(me + 1, replicas, greet)

    loads[3].wait()
    loads[4].wait()
    for c in range(chunks):
        restore(c)

    def name(n, t):
        for s in range(fold):
            lines = slice(s * groups, (s + 1) * groups)
            lanes = slice(s * topk, (s + 1) * topk)
            named = jnp.concatenate([all_ids[t, r].astype(jnp.int32)[:, lanes] for r in range(team)], axis=1)
            span_a[n, lines, :] = (named // BLOCK).astype(F32)
            span_b[n, lines, :] = (named % BLOCK).astype(F32)

    def gather(n, t, p):
        for s in range(fold):
            lines = slice(s * groups + p * half, s * groups + (p + 1) * half)
            lanes = slice(s * topk, (s + 1) * topk)
            span_v[n, lines, :] = jnp.concatenate([all_values[p, t, r].astype(F32)[:, lanes] for r in range(team)], axis=1)

    def densify(n, c, energy):
        tiles = []
        for s in range(fold):
            lines = pl.ds(s * groups + c * SUBLANES, SUBLANES)
            tiles.append([ref[n, lines, :] for ref in (span_a, span_b, span_v)])
        for u, g in enumerate(members(c)):
            blocks = []
            for s in range(fold):
                a, b, v = (tile[u:u + 1].astype(BF16) for tile in tiles[s])
                row_hot = jnp.where(level == a, v, zero)
                col_hot = jnp.where(level == b, one, zero)
                block = dot_nt(row_hot, col_hot)
                if n:
                    block = block + partial[g * fold + s]
                if n + 1 < teams:
                    partial[g * fold + s] = block
                blocks.append(block)
            if n + 1 == teams:
                combined = jnp.concatenate(blocks, axis=1)
                mixed[g] = combined.astype(BF16)
                energy = energy + jnp.sum((combined * combined).reshape(BLOCK // SUBLANES, SUBLANES, width), axis=0)
        return energy

    energy = jnp.zeros((SUBLANES, width), F32)
    below = (home + teams - 1) // teams
    first = home - below * (1 - 2 * own // team)
    for n in range(teams):
        t = lax.rem(first + n, teams)
        bulk(all_ids.at[t], id_sem.at[0], id_in.at[t]).wait_recv()
        name(n, t)
        for p in range(parts):
            bulk(all_values.at[p, t], value_sem.at[p], value_in.at[p, t]).wait_recv()
            gather(n, t, p)
            for c in range(p * half // SUBLANES, (p + 1) * half // SUBLANES):
                energy = densify(n, c, energy)

    energy = sum(energy[:, n * LANES:(n + 1) * LANES] for n in range(width // LANES))
    e_out[...] = energy
    e_in[part] = energy

    def copy_tp(k, slot):
        return pltpu.make_async_remote_copy(
            src_ref=e_out, dst_ref=e_in.at[slot],
            send_sem=e_send.at[k], recv_sem=e_recv.at[k], **mate(k),
        )

    each(1, shards, lambda k: copy_tp(k, part).start())
    for c in range(chunks - 1):
        tiles = decode([mixed[g] for g in members(c)], deep[...], rows[...])
        for g, tile in zip(members(c), tiles):
            dense_ref[:, columns(g, width)] = tile
    for u, g in enumerate(members(chunks - 1)):
        last_ref[u] = mixed[g]
    basis_ref[...] = rows[...]
    deep_ref[...] = deep[...]
    for n in range(teams):
        slots = pl.ds(0, team if n else team - 1)
        bulk(all_ids.at[n, slots], id_sem.at[0], id_in.at[n]).wait_send()
        for p in range(parts):
            bulk(all_values.at[p, n, slots], value_sem.at[p], value_in.at[p, n]).wait_send()
    each(1, shards, lambda k: copy_tp(k, lax.rem(part - k + shards, shards)).wait())


def finish(total, newm_ref, dense_ref, e_ref, last_ref, deep_ref, rows_ref, newm_hbm, upd_hbm, upd, sems):
    pieces = sems.shape[0] - 1
    stretch = upd.shape[1] // pieces
    done = dense_ref.shape[1] // stretch
    first = pltpu.make_async_copy(newm_ref, newm_hbm, sems.at[pieces])
    first.start()
    tiles = decode([last_ref[u] for u in range(last_ref.shape[0])], deep_ref[...], rows_ref[...])
    mean = jnp.sum(e_ref[...]) / total
    scale = lax.rsqrt(jnp.full((1, stretch), mean + EPSILON, F32))
    copies = []
    for n in range(pieces):
        cols = pl.ds(n * stretch, stretch)
        block = dense_ref[:, cols] if n < done else jnp.concatenate(tiles, axis=1)
        upd[:, cols] = (block * scale).astype(BF16)
        copies.append(pltpu.make_async_copy(upd.at[:, cols], upd_hbm.at[:, cols], sems.at[n]))
        copies[-1].start()
    first.wait()
    for copy in copies:
        copy.wait()


def local(gradient, momentum, indices, replicas, shards):
    height, cols = gradient.shape[1:]
    topk = indices.shape[-1]
    fold = LANES // topk
    spans = cols // BLOCK
    groups = spans // fold
    width = fold * BLOCK
    chunks = groups // SUBLANES
    assert height == BLOCK and chunks * SUBLANES * fold == spans and width == 2 * LANES
    basis = dct_basis(BLOCK)
    pair = np.eye(2, dtype=np.float32)
    both = [np.concatenate(np_halves(np.kron(pair, w)), axis=1) for w in (basis.T, basis)]
    fwd, inv = (jnp.asarray(np.concatenate([w, w], axis=0)) for w in both)
    deep = jnp.asarray(np.concatenate(np_halves(np.kron(np.eye(fold, dtype=np.float32), basis)), axis=0))
    rows = jnp.asarray(np.concatenate(np_halves(basis.T), axis=1))
    team = min(replicas, 2 * LANES // topk)
    teams = replicas // team
    parts = 1
    depth = team * topk
    assert teams * team == replicas and depth % LANES == 0
    vmem = pl.BlockSpec(memory_space=pltpu.VMEM)
    hbm = pl.BlockSpec(memory_space=pltpu.HBM)
    half = pltpu.VMEM((SUBLANES, height, width), BF16)
    operands = (gradient[0], momentum[0], indices.reshape(spans, topk).T, fwd, inv, deep, rows)
    newm, *rest = pl.pallas_call(
        functools.partial(kernel, replicas, shards),
        out_shape=(
            jax.ShapeDtypeStruct((height, cols), BF16),
            jax.ShapeDtypeStruct((height, cols - SUBLANES * width), F32),
            jax.ShapeDtypeStruct((shards, SUBLANES, LANES), F32),
            jax.ShapeDtypeStruct((SUBLANES, height, width), BF16),
            jax.ShapeDtypeStruct(deep.shape, BF16),
            jax.ShapeDtypeStruct(rows.shape, BF16),
        ),
        in_specs=[hbm] * 7,
        out_specs=(vmem,) * 6,
        scratch_shapes=[
            pltpu.VMEM((height, cols), BF16),
            pltpu.VMEM((height, cols), BF16),
            pltpu.VMEM((topk, spans), jnp.int32),
            pltpu.VMEM(fwd.shape, BF16),
            pltpu.VMEM(inv.shape, BF16),
            pltpu.VMEM(deep.shape, BF16),
            pltpu.VMEM(rows.shape, BF16),
            pltpu.VMEM((spans, topk), jnp.int32),
            pltpu.VMEM((2, groups, LANES), F32),
            half, half, half, half,
            pltpu.VMEM((height, groups * 2 * LANES), BF16),
            pltpu.VMEM((groups, LANES), jnp.int16),
            pltpu.VMEM((teams, team, groups, LANES), jnp.int16),
            pltpu.VMEM((groups, LANES), F32),
            pltpu.VMEM((parts, groups // parts, LANES), BF16),
            pltpu.VMEM((parts, teams, team, groups // parts, LANES), BF16),
            pltpu.VMEM((teams, spans, depth), F32),
            pltpu.VMEM((teams, spans, depth), F32),
            pltpu.VMEM((teams, spans, depth), F32),
            pltpu.VMEM((spans, height, BLOCK), F32),
            pltpu.VMEM((groups, height, width), BF16),
            pltpu.VMEM((SUBLANES, LANES), F32),
            pltpu.SemaphoreType.DMA((2, chunks)),
            pltpu.SemaphoreType.DMA((5,)),
            pltpu.SemaphoreType.DMA((1,)),
            pltpu.SemaphoreType.DMA((parts,)),
            pltpu.SemaphoreType.DMA((teams,)),
            pltpu.SemaphoreType.DMA((parts, teams)),
            pltpu.SemaphoreType.REGULAR((replicas,)),
            pltpu.SemaphoreType.DMA((shards,)),
            pltpu.SemaphoreType.DMA((shards,)),
        ],
        compiler_params=pltpu.CompilerParams(
            collective_id=0, has_side_effects=True, vmem_limit_bytes=24 * 2 ** 20
        ),
        name="demo_step",
    )(*(pltpu.with_memory_space_constraint(x, pltpu.HBM) for x in operands))
    newm, update = pl.pallas_call(
        functools.partial(finish, float(height * cols * shards)),
        out_shape=(
            jax.ShapeDtypeStruct((height, cols), BF16),
            jax.ShapeDtypeStruct((height, cols), BF16),
        ),
        in_specs=[vmem] * 6,
        out_specs=(hbm, hbm),
        scratch_shapes=[pltpu.VMEM((height, cols), BF16), pltpu.SemaphoreType.DMA((chunks + 1,))],
        compiler_params=pltpu.CompilerParams(vmem_limit_bytes=8 * 2 ** 20),
        name="finish",
    )(newm, *rest)
    return newm[None], update


def solution(mesh):
    in_specs = (P("dp", "tensor", None), P("dp", "tensor", None), P("dp", "tensor", None, None))
    out_specs = (P("dp", "tensor", None), P("tensor", None))
    body = functools.partial(local, replicas=mesh.shape["dp"], shards=mesh.shape["tensor"])
    return jax.shard_map(body, mesh=mesh, in_specs=in_specs, out_specs=out_specs, check_vma=False)
```

```python
import functools

import jax
import jax.numpy as jnp
import numpy as np
from jax import lax
from jax.experimental import pallas as pl
from jax.experimental.pallas import tpu as pltpu
from jax.sharding import PartitionSpec as P

BLOCK = 64
LANES = 128
SUBLANES = 8
EPSILON = 1e-06
DECAY = 0.999
GAIN = 1.3725
F32 = jnp.float32
BF16 = jnp.bfloat16
MESH = pl.DeviceIdType.MESH


def dct_basis(edge):
    frequency = np.arange(edge, dtype=np.float64)[:, None]
    position = np.arange(edge, dtype=np.float64)[None, :]
    waves = np.cos(np.pi * (2.0 * position + 1.0) * frequency / (2.0 * edge))
    weights = np.where(frequency == 0.0, np.sqrt(1.0 / edge), np.sqrt(2.0 / edge))
    return (waves * weights).astype(np.float32)


def halves(x):
    high = x.astype(BF16)
    return high, (x - high.astype(F32)).astype(BF16)


def np_halves(x):
    high = x.astype(jnp.bfloat16)
    return high, (x - high.astype(np.float32)).astype(jnp.bfloat16)


def dot(a, b):
    return jnp.dot(a, b, preferred_element_type=F32)


def dot_nt(a, b):
    return lax.dot_general(a, b, (((1,), (1,)), ((), ())), preferred_element_type=F32)


def wide(blocks, weights):
    tiles = [block[:, n * LANES:(n + 1) * LANES] for block in blocks for n in range(2)]
    high, low = halves(jnp.concatenate(tiles, axis=0))
    both = dot(jnp.concatenate([high, low], axis=1), weights)
    out = both[:, :LANES] + both[:, LANES:]
    parts = [out[n * BLOCK:(n + 1) * BLOCK] for n in range(len(tiles))]
    return [jnp.concatenate(parts[2 * n:2 * n + 2], axis=1) for n in range(len(blocks))]


def decode(blocks, deep, rows):
    stack = jnp.concatenate(blocks, axis=0)
    across = dot(stack, deep).astype(BF16)
    parts = [across[u * BLOCK:(u + 1) * BLOCK] for u in range(len(blocks))]
    return [dot(rows, jnp.concatenate([part, part], axis=0)) for part in parts]


def kernel(
    replicas, shards,
    grad_hbm, mom_hbm, idx_hbm, fwd_hbm, inv_hbm, deep_hbm, rows_hbm,
    newm_ref, dense_ref, e_in, last_ref, deep_ref, basis_ref,
    grad, mom, idx, fwd, inv, deep, rows,
    by_span, picks, high_even, low_even, high_odd, low_odd, factor,
    ids, all_ids, values, shipped, all_values, span_a, span_b, span_v, partial, mixed, e_out,
    x_sem, c_sem, id_sem, value_sem, id_in, twin_in, value_in, ready, e_send, e_recv,
):
    me = lax.axis_index("dp")
    part = lax.axis_index("tensor")
    barrier = pltpu.get_barrier_semaphore()

    topk, spans = idx.shape
    fold = LANES // topk
    width = fold * BLOCK
    groups = spans // fold
    chunks = groups // SUBLANES
    stretch = SUBLANES * width
    team = all_ids.shape[1]
    teams = replicas // team
    depth = team * topk
    home = me // team
    parts, half = shipped.shape[:2]
    own = lax.rem(me, team)

    loads = [pltpu.make_async_copy(src, dst, c_sem.at[n]) for n, (src, dst) in enumerate(
        [(idx_hbm, idx), (fwd_hbm, fwd), (rows_hbm, rows), (inv_hbm, inv), (deep_hbm, deep)])]

    def slab(c):
        cols = pl.ds(c * stretch, stretch)
        return [pltpu.make_async_copy(src.at[:, cols], dst.at[:, cols], x_sem.at[n, c])
                for n, (src, dst) in enumerate([(mom_hbm, mom), (grad_hbm, grad)])]

    loads[0].start()
    loads[1].start()
    for copy in slab(0):
        copy.start()
    loads[2].start()
    for c in range(1, chunks):
        for copy in slab(c):
            copy.start()
    loads[3].start()
    loads[4].start()

    def each(low, high, act):
        def step(k, c):
            act(k)
            return c
        lax.fori_loop(low, high, step, 0)

    def peer(j):
        return dict(device_id={"dp": j}, device_id_type=MESH)

    def mate(k):
        return dict(device_id={"tensor": lax.rem(part + k, shards)}, device_id_type=MESH)

    each(me + 1, replicas, lambda j: pl.semaphore_signal(barrier, inc=1, **peer(j)))
    each(1, shards, lambda k: pl.semaphore_signal(barrier, inc=1, **mate(k)))
    pl.semaphore_wait(barrier, me + shards - 1)
    each(0, me, lambda j: pl.semaphore_signal(ready.at[me], inc=1, **peer(j)))

    loads[0].wait()
    by_span[...] = idx[...].T
    chosen = jnp.concatenate(
        [by_span[pl.ds(s, groups, stride=fold), :] for s in range(fold)], axis=1
    )
    ids[...] = chosen.astype(jnp.int16)
    picks[0] = (chosen // BLOCK).astype(F32)
    slot = lax.broadcasted_iota(jnp.int32, chosen.shape, 1) // topk
    picks[1] = (chosen % BLOCK + BLOCK * slot).astype(F32)

    zero = jnp.zeros((), BF16)
    one = jnp.ones((), BF16)
    tall = lax.broadcasted_iota(jnp.int32, (width, LANES), 0).astype(F32).astype(BF16)
    short = lax.broadcasted_iota(jnp.int32, (BLOCK, LANES), 0).astype(F32).astype(BF16)
    level = lax.broadcasted_iota(jnp.int32, (BLOCK, depth), 0).astype(F32).astype(BF16)

    def hot(levels, plane, g):
        return jnp.where(levels == picks[plane, pl.ds(g, 1), :].astype(BF16), one, zero)

    def columns(g, size):
        return pl.ds(pl.multiple_of(g * size, size), size)

    def members(c):
        return range(c * SUBLANES, (c + 1) * SUBLANES)

    def renew(g):
        cols = columns(g, width)
        return DECAY * mom[:, cols].astype(F32) + grad[:, cols].astype(F32)

    highs, lows = (high_even, high_odd), (low_even, low_odd)

    def transform(c):
        high, low = highs[c % 2], lows[c % 2]
        for u, block in enumerate(wide([renew(g) for g in members(c)], fwd[...])):
            high[u], low[u] = halves(block)

    def pick(c):
        high, low = highs[c % 2], lows[c % 2]
        for u, g in enumerate(members(c)):
            both = dot(jnp.concatenate([high[u], low[u]], axis=0), hot(tall, 1, g))
            row_hot = hot(short, 0, g)
            waves = dot(rows[...], jnp.concatenate([row_hot, row_hot], axis=0))
            value = jnp.sum((both[:BLOCK] + both[BLOCK:]) * waves, axis=0, keepdims=True)
            values[pl.ds(g, 1), :] = value
            factor[:, columns(g, 2 * LANES)] = jnp.concatenate(halves(waves * value), axis=1)

    def restore(c):
        spread = []
        batch = [c * SUBLANES + u for u in range(SUBLANES)]
        for g in batch:
            col_hot = hot(tall, 1, g)
            spread.append(dot_nt(factor[:, columns(g, 2 * LANES)], jnp.concatenate([col_hot, col_hot], axis=1)))
        for g, block in zip(batch, wide(spread, inv[...])):
            newm_ref[:, columns(g, width)] = (renew(g) - block).astype(BF16)

    def send(src, dst, send_sem, recv_sem, j):
        pltpu.make_async_remote_copy(
            src_ref=src, dst_ref=dst.at[home, own], send_sem=send_sem, recv_sem=recv_sem.at[home], **peer(j),
        ).start()

    def send_ids(arrivals, j):
        send(ids, all_ids, id_sem.at[0], arrivals, j)

    def twin(t):
        return t * team + own

    def forward(t):
        src = all_ids.at[t, own]
        bulk(src, id_sem.at[0], twin_in.at[t]).wait_recv()

        def pass_on(j):
            pltpu.make_async_remote_copy(
                src_ref=src, dst_ref=src, send_sem=id_sem.at[0], recv_sem=id_in.at[t], **peer(j),
            ).start()

        each(home * team, me, pass_on)
        each(me + 1, (home + 1) * team, pass_on)

    def send_values(p, j):
        send(shipped.at[p], all_values.at[p], value_sem.at[p], value_in.at[p], j)

    def keep(src, dst, sem):
        pltpu.make_async_copy(src, dst.at[home, own], sem.at[home]).start()

    def greet(j):
        pl.semaphore_wait(ready.at[j], 1)
        for p in range(parts):
            send_values(p, j)

    def greet_mate(j):
        greet(j)
        send_ids(id_in, j)

    def greet_twin(t):
        greet(twin(t))
        send_ids(twin_in, twin(t))

    def greet_others(t):
        each(t * team, twin(t), greet)
        each(twin(t) + 1, (t + 1) * team, greet)

    def bulk(ref, send_sem, recv_sem):
        return pltpu.make_async_remote_copy(
            src_ref=ref, dst_ref=ref, send_sem=send_sem, recv_sem=recv_sem, **peer(me),
        )

    each(0, home, lambda t: send_ids(twin_in, twin(t)))
    each(home * team, me, functools.partial(send_ids, id_in))
    keep(ids, all_ids, id_in)

    loads[1].wait()
    for copy in slab(0):
        copy.wait()
    transform(0)
    loads[2].wait()
    for c in range(chunks):
        if c + 1 < chunks:
            for copy in slab(c + 1):
                copy.wait()
            transform(c + 1)
        pick(c)
        p = (c + 1) * SUBLANES // half - 1
        if (c + 1) * SUBLANES == (p + 1) * half:
            shipped[p] = values[pl.ds(p * half, half), :].astype(BF16)
            each(0, me, functools.partial(send_values, p))
            keep(shipped.at[p], all_values.at[p], value_in.at[p])
    each(home + 1, teams, greet_twin)
    each(me + 1, (home + 1) * team, greet_mate)
    loads[3].wait()
    loads[4].wait()
    early = chunks // (1 + me)
    each(0, early, restore)
    each(home + 1, teams, greet_others)
    each(home + 1, teams, forward)
    each(early, chunks, restore)
    each(0, home, forward)

    def name(n, t):
        for s in range(fold):
            lines = slice(s * groups, (s + 1) * groups)
            lanes = slice(s * topk, (s + 1) * topk)
            named = jnp.concatenate([all_ids[t, r].astype(jnp.int32)[:, lanes] for r in range(team)], axis=1)
            span_a[n, lines, :] = (named // BLOCK).astype(F32)
            span_b[n, lines, :] = (named % BLOCK).astype(F32)

    def gather(n, t, p):
        for s in range(fold):
            lines = slice(s * groups + p * half, s * groups + (p + 1) * half)
            lanes = slice(s * topk, (s + 1) * topk)
            span_v[n, lines, :] = jnp.concatenate([all_values[p, t, r].astype(F32)[:, lanes] for r in range(team)], axis=1)

    def densify(n, c, energy):
        tiles = []
        for s in range(fold):
            lines = pl.ds(s * groups + c * SUBLANES, SUBLANES)
            tiles.append([ref[n, lines, :] for ref in (span_a, span_b, span_v)])
        for u, g in enumerate(members(c)):
            blocks = []
            for s in range(fold):
                a, b, v = (tile[u:u + 1].astype(BF16) for tile in tiles[s])
                row_hot = jnp.where(level == a, v, zero)
                col_hot = jnp.where(level == b, one, zero)
                blocks.append(dot_nt(row_hot, col_hot))
            combined = jnp.concatenate(blocks, axis=1)
            if n:
                combined = combined + partial[g]
            if n + 1 < teams:
                partial[g] = combined
            else:
                mixed[g] = combined.astype(BF16)
                energy = energy + jnp.sum((combined * combined).reshape(BLOCK // SUBLANES, SUBLANES, width), axis=0)
        return energy

    energy = jnp.zeros((SUBLANES, width), F32)
    for n in range(teams):
        t = lax.rem(home + n, teams)
        bulk(all_ids.at[t, pl.ds(0, team - 1 if n else team)], id_sem.at[0], id_in.at[t]).wait_recv()
        name(n, t)
        for p in range(parts):
            bulk(all_values.at[p, t], value_sem.at[p], value_in.at[p, t]).wait_recv()
            gather(n, t, p)
            for c in range(p * half // SUBLANES, (p + 1) * half // SUBLANES):
                energy = densify(n, c, energy)

    energy = sum(energy[:, n * LANES:(n + 1) * LANES] for n in range(width // LANES))
    e_out[...] = energy
    e_in[part] = energy

    def copy_tp(k, slot):
        return pltpu.make_async_remote_copy(
            src_ref=e_out, dst_ref=e_in.at[slot],
            send_sem=e_send.at[k], recv_sem=e_recv.at[k], **mate(k),
        )

    each(1, shards, lambda k: copy_tp(k, part).start())
    for c in range(chunks - 1):
        tiles = decode([mixed[g] for g in members(c)], deep[...], rows[...])
        for g, tile in zip(members(c), tiles):
            dense_ref[:, columns(g, width)] = tile
    for u, g in enumerate(members(chunks - 1)):
        last_ref[u] = mixed[g]
    basis_ref[...] = rows[...]
    deep_ref[...] = deep[...]
    for n in range(teams):
        slots = pl.ds(0, team if n else team - 1)
        bulk(all_ids.at[n, slots], id_sem.at[0], id_in.at[n]).wait_send()
        for p in range(parts):
            bulk(all_values.at[p, n, slots], value_sem.at[p], value_in.at[p, n]).wait_send()
    each(1, shards, lambda k: copy_tp(k, lax.rem(part - k + shards, shards)).wait())


def finish(total, newm_ref, dense_ref, e_ref, last_ref, deep_ref, rows_ref, newm_hbm, upd_hbm, upd, sems):
    pieces = sems.shape[0] - 1
    stretch = upd.shape[1] // pieces
    done = dense_ref.shape[1] // stretch
    first = pltpu.make_async_copy(newm_ref, newm_hbm, sems.at[pieces])
    first.start()
    mean = jnp.sum(e_ref[...]) / total
    scale = lax.rsqrt(jnp.full((1, stretch), mean + EPSILON, F32)) * (1.0 / GAIN)
    copies = []
    for n in range(pieces):
        cols = pl.ds(n * stretch, stretch)
        if n < done:
            block = dense_ref[:, cols]
        else:
            blocks = [last_ref[u] for u in range(last_ref.shape[0])]
            block = jnp.concatenate(decode(blocks, deep_ref[...], rows_ref[...]), axis=1)
        upd[:, cols] = (block * scale).astype(BF16)
        copies.append(pltpu.make_async_copy(upd.at[:, cols], upd_hbm.at[:, cols], sems.at[n]))
        copies[-1].start()
    first.wait()
    for copy in copies:
        copy.wait()


def local(gradient, momentum, indices, replicas, shards):
    height, cols = gradient.shape[1:]
    topk = indices.shape[-1]
    fold = LANES // topk
    spans = cols // BLOCK
    groups = spans // fold
    width = fold * BLOCK
    chunks = groups // SUBLANES
    assert height == BLOCK and chunks * SUBLANES * fold == spans and width == 2 * LANES
    basis = dct_basis(BLOCK)
    pair = np.eye(2, dtype=np.float32)
    both = [np.concatenate(np_halves(np.kron(pair, w)), axis=1) for w in (basis.T, basis)]
    fwd, inv = (jnp.asarray(np.concatenate([w, w], axis=0)) for w in both)
    deep = jnp.asarray(np.kron(np.eye(fold, dtype=np.float32), GAIN * basis).astype(jnp.bfloat16))
    rows = jnp.asarray(np.concatenate(np_halves(basis.T), axis=1))
    team = min(replicas, 2 * LANES // topk)
    teams = replicas // team
    parts = 1
    depth = team * topk
    assert teams * team == replicas and depth % LANES == 0
    vmem = pl.BlockSpec(memory_space=pltpu.VMEM)
    hbm = pl.BlockSpec(memory_space=pltpu.HBM)
    half = pltpu.VMEM((SUBLANES, height, width), BF16)
    operands = (gradient[0], momentum[0], indices.reshape(spans, topk).T, fwd, inv, deep, rows)
    newm, *rest = pl.pallas_call(
        functools.partial(kernel, replicas, shards),
        out_shape=(
            jax.ShapeDtypeStruct((height, cols), BF16),
            jax.ShapeDtypeStruct((height, cols - SUBLANES * width), F32),
            jax.ShapeDtypeStruct((shards, SUBLANES, LANES), F32),
            jax.ShapeDtypeStruct((SUBLANES, height, width), BF16),
            jax.ShapeDtypeStruct(deep.shape, BF16),
            jax.ShapeDtypeStruct(rows.shape, BF16),
        ),
        in_specs=[hbm] * 7,
        out_specs=(vmem,) * 6,
        scratch_shapes=[
            pltpu.VMEM((height, cols), BF16),
            pltpu.VMEM((height, cols), BF16),
            pltpu.VMEM((topk, spans), jnp.int32),
            pltpu.VMEM(fwd.shape, BF16),
            pltpu.VMEM(inv.shape, BF16),
            pltpu.VMEM(deep.shape, BF16),
            pltpu.VMEM(rows.shape, BF16),
            pltpu.VMEM((spans, topk), jnp.int32),
            pltpu.VMEM((2, groups, LANES), F32),
            half, half, half, half,
            pltpu.VMEM((height, groups * 2 * LANES), BF16),
            pltpu.VMEM((groups, LANES), jnp.int16),
            pltpu.VMEM((teams, team, groups, LANES), jnp.int16),
            pltpu.VMEM((groups, LANES), F32),
            pltpu.VMEM((parts, groups // parts, LANES), BF16),
            pltpu.VMEM((parts, teams, team, groups // parts, LANES), BF16),
            pltpu.VMEM((teams, spans, depth), F32),
            pltpu.VMEM((teams, spans, depth), F32),
            pltpu.VMEM((teams, spans, depth), F32),
            pltpu.VMEM((groups, height, width), F32),
            pltpu.VMEM((groups, height, width), BF16),
            pltpu.VMEM((SUBLANES, LANES), F32),
            pltpu.SemaphoreType.DMA((2, chunks)),
            pltpu.SemaphoreType.DMA((5,)),
            pltpu.SemaphoreType.DMA((1,)),
            pltpu.SemaphoreType.DMA((parts,)),
            pltpu.SemaphoreType.DMA((teams,)),
            pltpu.SemaphoreType.DMA((teams,)),
            pltpu.SemaphoreType.DMA((parts, teams)),
            pltpu.SemaphoreType.REGULAR((replicas,)),
            pltpu.SemaphoreType.DMA((shards,)),
            pltpu.SemaphoreType.DMA((shards,)),
        ],
        compiler_params=pltpu.CompilerParams(
            collective_id=0, has_side_effects=True, vmem_limit_bytes=24 * 2 ** 20
        ),
        name="demo_step",
    )(*(pltpu.with_memory_space_constraint(x, pltpu.HBM) for x in operands))
    newm, update = pl.pallas_call(
        functools.partial(finish, float(height * cols * shards)),
        out_shape=(
            jax.ShapeDtypeStruct((height, cols), BF16),
            jax.ShapeDtypeStruct((height, cols), BF16),
        ),
        in_specs=[vmem] * 6,
        out_specs=(hbm, hbm),
        scratch_shapes=[pltpu.VMEM((height, cols), BF16), pltpu.SemaphoreType.DMA((chunks + 1,))],
        compiler_params=pltpu.CompilerParams(vmem_limit_bytes=8 * 2 ** 20),
        name="finish",
    )(newm, *rest)
    return newm[None], update


def solution(mesh):
    in_specs = (P("dp", "tensor", None), P("dp", "tensor", None), P("dp", "tensor", None, None))
    out_specs = (P("dp", "tensor", None), P("tensor", None))
    body = functools.partial(local, replicas=mesh.shape["dp"], shards=mesh.shape["tensor"])
    return jax.shard_map(body, mesh=mesh, in_specs=in_specs, out_specs=out_specs, check_vma=False)
```
